32 devices in a mesh: groups: 2 (over x), feat: 16 (over z, y, core).
Axes of the slice: x: 2, y: 2, z: 4, core: 2. Of those that a mesh axis runs over, the one named last changes fastest.
Arguments:
- cells: bfloat16 [96, 512, 192], P('groups', 'feat'), parts along dimension 0, may hold values from -6 to 6
- missing: int32 [96, 512], P('groups', 'feat'), parts along dimension 0, may hold values 0 or 1
- feat_ids: int32 [1024], P(('groups', 'feat')), parts along dimension 0, may hold values from 0 to 63
- feat_table: float32 [64, 192], replicated, may hold values from -5 to 5
- nan_embed: float32 [192], replicated, may hold values from -5 to 5
- gain_one: float32 [192], replicated, may hold values from 0.1 to 1.9
- w_qkv: bfloat16 [192, 576], replicated, may hold values from -3 to 3
- w_out: bfloat16 [192, 192], replicated, may hold values from -0.4375 to 0.4375
- gain_two: float32 [192], replicated, may hold values from 0.1 to 1.9
- w_up: bfloat16 [192, 768], replicated, may hold values from -0.4375 to 0.4375
- w_down: bfloat16 [768, 192], replicated, may hold values from -0.21875 to 0.21875
Outputs:
- result: float32 [96, 512, 192], P('groups', 'feat'), parts along dimension 0
The draws below stay inside these ranges and needn't reach their ends.
There are 2 independent parts, one for each index of `groups`. The reference program is written for one: setup_inputs(seed, part) draws one part's arguments, and reference() takes and returns one part's arrays. A program takes and returns all parts, laid end to end along the dimension named above; an argument that names none is the same for every part. Nothing has to cross between parts.
All inputs are finite; a program needn't handle non-finite values. No bound on the sum of `missing` on one device may be relied on, other than what follows from the above.
Results may differ from the reference program's by a relative error of at most 0.007.
The reference program's roundings to bfloat16 on the way (of `tokens`, `normed`, `qkv`, `probs`, `context`, `normed_two` and `act`) count: a program that leaves them out, or rounds other values in their place, can miss the bound.
Values may be sent and summed in bfloat16 or wider, within the bound.
A program may use at most 64 MiB of HBM per device.

```python
import jax
import jax.numpy as jnp
from jax import lax

E = 192
HEADS = 6
MLP = 768
F = 512
NCAT = 64
R = 48


def draw_w_qkv(key, part):
    weights = jax.random.normal(key, (E, 3 * E), jnp.float32) * E ** (-0.5)
    return jnp.clip(weights, -3.0, 3.0).astype(jnp.bfloat16)


def touch_ends(values, key, smallest, top_value):
    longest = values.shape.index(max(values.shape))
    spots = []
    for shift in (0, 1):
        where = [jax.random.randint(jax.random.fold_in(key, axis), (), 0, length) for axis, length in enumerate(values.shape)]
        where[longest] = (where[longest] + shift) % values.shape[longest]
        spots.append(tuple(where))
    return values.at[spots[0]].set(smallest).at[spots[1]].set(top_value)


def block_scale(rng, extent, shards, smallest, high):
    def one(dim, parts):
        steps = jax.random.uniform(jax.random.fold_in(jax.random.fold_in(rng, 6), dim), (parts,), jnp.float32, smallest / len(shards), high / len(shards))
        return jnp.repeat(jnp.exp(steps), extent[dim] // parts).reshape((-1,) + (1,) * (len(extent) - dim - 1))

    loudness = one(*shards[0])
    for cut in shards[1:]:
        loudness = loudness * one(*cut)
    return loudness


def centred(stream_key, extent, spread, reach, pieces=(), held_as=jnp.bfloat16):
    drawn = jax.random.normal(stream_key, extent, jnp.float32) * spread
    if len(pieces) > 0:
        drawn = block_scale(stream_key, extent, pieces, -0.22, 0.18) * drawn
    return jnp.clip(drawn, min=-reach, max=reach).astype(held_as)


def setup_inputs(seed: int = 0, part: int = 0) -> dict:
    streams_of = jax.random.split(jax.random.key(seed), 12)
    part_splits = jax.random.split(jax.random.fold_in(streams_of[11], part), 12)
    return {
        "cells": centred(part_splits[0], (R, F, E), 1.0, 6.0, ((1, 16),)),
        "missing": touch_ends((jax.random.randint(part_splits[1], (R, F), 0, 4) < 1).astype(jnp.int32), jax.random.fold_in(part_splits[1], 1), 0, 1),
        "feat_ids": touch_ends(jax.random.randint(part_splits[2], (F,), 0, NCAT), jax.random.fold_in(part_splits[2], 1), 0, NCAT - 1).astype(jnp.int32),
        "feat_table": centred(streams_of[3], (NCAT, E), 0.7, 5.0, (), jnp.float32),
        "nan_embed": centred(streams_of[4], (E,), 1.0, 5.0, (), jnp.float32),
        "gain_one": jnp.clip(1.0 + 0.18 * jax.random.normal(streams_of[5], (E,), jnp.float32), 0.1, 1.9),
        "w_qkv": draw_w_qkv(jax.random.fold_in(streams_of[11], 71), part),
        "w_out": centred(streams_of[7], (E, E), E ** -0.5, 0.4375),
        "gain_two": jnp.clip(1.0 + 0.18 * jax.random.normal(streams_of[8], (E,), jnp.float32), 0.1, 1.9),
        "w_up": centred(streams_of[9], (E, MLP), E ** -0.5, 0.4375),
        "w_down": centred(streams_of[10], (MLP, E), MLP ** -0.5, 0.21875),
    }


def cell_norm(values, gain):
    mean = lax.optimization_barrier(jnp.mean(values, axis=-1, keepdims=True))
    centered = values - mean
    var = lax.optimization_barrier(jnp.mean(centered * centered, axis=-1, keepdims=True))
    return centered * lax.rsqrt(var + 1e-05) * gain

def attend(qkv):
    width = qkv.shape[-1] // 3
    count = qkv.shape[0]
    head_dim = width // HEADS
    query = qkv[:, :width].reshape(count, HEADS, head_dim).astype(jnp.float32)
    keys = qkv[:, width:2 * width].reshape(count, HEADS, head_dim).astype(jnp.float32)
    values = qkv[:, 2 * width:].reshape(count, HEADS, head_dim).astype(jnp.float32)
    scores = jnp.einsum('qhd,phd->hqp', query, keys) * head_dim ** (-0.5)
    top = lax.optimization_barrier(jnp.max(scores, axis=-1, keepdims=True))
    expo = jnp.exp(scores - top)
    probs = (expo / lax.optimization_barrier(jnp.sum(expo, axis=-1, keepdims=True))).astype(jnp.bfloat16)
    context = jnp.einsum('hqp,phd->qhd', probs.astype(jnp.float32), values)
    return context.astype(jnp.bfloat16).reshape(count, width)

def reference(cells, missing, feat_ids, feat_table, nan_embed, gain_one, w_qkv, w_out, gain_two, w_up, w_down):
    onehot = (feat_ids[:, None] == jnp.arange(NCAT, dtype=jnp.int32)[None, :]).astype(jnp.float32)
    femb = jnp.dot(onehot, feat_table, precision=lax.Precision.HIGHEST)
    tokens = (cells.astype(jnp.float32) + missing[..., None].astype(jnp.float32) * nan_embed + femb[None]).astype(jnp.bfloat16)

    def one_row(row):
        base = row.astype(jnp.float32)
        normed = cell_norm(base, gain_one).astype(jnp.bfloat16)
        qkv = jnp.dot(normed, w_qkv, preferred_element_type=jnp.float32).astype(jnp.bfloat16)
        context = attend(qkv)
        mid = base + jnp.dot(context, w_out, preferred_element_type=jnp.float32)
        normed_two = cell_norm(mid, gain_two).astype(jnp.bfloat16)
        act = jax.nn.gelu(jnp.dot(normed_two, w_up, preferred_element_type=jnp.float32), approximate=False).astype(jnp.bfloat16)
        return mid + jnp.dot(act, w_down, preferred_element_type=jnp.float32)
    return lax.map(one_row, tokens)
```

```python
import functools
import math

import jax
import jax.numpy as jnp
from jax import lax
from jax.experimental import pallas as pl
from jax.experimental.pallas import tpu as pltpu
from jax.sharding import PartitionSpec as P

HEADS = 6
MESH = pl.DeviceIdType.MESH
F32 = jnp.float32
BF16 = jnp.bfloat16
LIMIT = 60 * 1024 * 1024


def cell_norm(values, gain):
    mean = jnp.mean(values, axis=-1, keepdims=True)
    centered = values - mean
    var = jnp.mean(centered * centered, axis=-1, keepdims=True)
    return (centered * lax.rsqrt(var + 1e-05) * gain).astype(BF16)


def pack(values, packed):
    if not packed:
        return values
    half = values.shape[-2] // 2
    tail = values[..., 128:]
    tail = jnp.concatenate([tail[..., :half, :], tail[..., half:, :]], axis=-1)
    return jnp.concatenate([values[..., :128], tail], axis=-2)


def unpack(values, feats, width, packed):
    if packed:
        rest = width - 128
        tail = values[:, feats:]
        tail = jnp.concatenate([tail[..., :rest], tail[..., rest:]], axis=-2)
        values = jnp.concatenate([values[:, :feats], tail], axis=-1)
    return values.reshape(values.shape[0] * feats, width)


def attend(normed, wk, wqv_t):
    width = wk.shape[0]
    head_dim = width // HEADS
    count = normed.shape[0]
    keys = jnp.dot(normed, wk, preferred_element_type=F32).astype(BF16)
    turned = lax.dot_general(
        wqv_t, normed, (((1,), (1,)), ((), ())), preferred_element_type=F32
    ).astype(BF16)
    scale = head_dim ** (-0.5) * math.log2(math.e)
    ones = jnp.ones((16, count), BF16)
    outs = []
    for head in range(HEADS):
        low = head * head_dim
        block = low // 128 * 128
        high = min(block + 128, width)
        parts = []
        if low > block:
            parts.append(jnp.zeros((low - block, count), BF16))
        parts.append(turned[low : low + head_dim])
        if high > low + head_dim:
            parts.append(jnp.zeros((high - low - head_dim, count), BF16))
        query = jnp.concatenate(parts, axis=0)
        scores = jnp.dot(keys[:, block:high], query, preferred_element_type=F32)
        top = jnp.max(scores, axis=0, keepdims=True)
        expo = jnp.exp2((scores - top) * scale).astype(BF16)
        values = jnp.concatenate([turned[width + low : width + low + head_dim], ones], axis=0)
        sums = jnp.dot(values, expo, preferred_element_type=F32)
        outs.append(sums[:head_dim] / sums[head_dim : head_dim + 1])
    return jnp.concatenate(outs, axis=0).T


def kernel(n, rows, feats, width, packed, *refs):
    sources, refs = refs[:11], refs[11:]
    out, held, refs = refs[0], refs[1:12], refs[12:]
    tok, got, ctx, back, wqv_t, done, load_sems, send_sems, recv_sems, out_sems = refs
    (cells, missing, feat_ids, feat_table, nan_embed) = held[:5]
    (gain_one, w_qkv, w_out, gain_two, w_up, w_down) = held[5:]
    me = lax.axis_index("feat")
    barrier = pltpu.get_barrier_semaphore()

    def greet(step, carry):
        peer = lax.rem(me + step, n)
        pl.semaphore_signal(barrier, inc=1, device_id={"feat": peer}, device_id_type=MESH)
        return carry

    lax.fori_loop(1, n, greet, 0)

    loads = [
        pltpu.make_async_copy(source, target, load_sems.at[spot])
        for spot, (source, target) in enumerate(zip(sources, held))
    ]
    for load in loads:
        load.start()
    for load in loads[:5]:
        load.wait()

    ncat = feat_table.shape[0]
    hot = (lax.broadcasted_iota(jnp.int32, (ncat, feats), 0) == feat_ids[...]).astype(F32)
    femb = lax.dot_general(
        hot, feat_table[...], (((0,), (0,)), ((), ())),
        precision=lax.Precision.HIGHEST, preferred_element_type=F32,
    )
    nan = nan_embed[...]
    absent = missing[...].astype(F32)
    def spread(source, target, kind, row):
        def one(step, carry):
            peer = lax.rem(me + step, n)
            pltpu.make_async_remote_copy(
                src_ref=source.at[row, peer],
                dst_ref=target.at[row, me],
                send_sem=send_sems.at[kind, row],
                recv_sem=recv_sems.at[kind, row],
                device_id={"feat": peer},
                device_id_type=MESH,
            ).start()
            return carry

        lax.fori_loop(1, n, one, 0)

    def settle(ref, sems, kind, row):
        piece = ref.at[row, pl.ds(0, n - 1)]
        pltpu.make_async_copy(piece, piece, sems.at[kind, row]).wait()

    for row in range(rows):
        for peer in range(n):
            spot = peer * rows + row
            values = cells[peer, row].astype(F32)
            values = (values + absent[:, spot : spot + 1] * nan + femb).astype(BF16)
            tok[row, peer] = pack(values, packed)
        if row == 0:
            pl.semaphore_wait(barrier, n - 1)
        spread(tok, got, 0, row)
    for row in range(rows):
        got[row, pl.ds(me, 1)] = tok[row, pl.ds(me, 1)]
    for load in loads[5:]:
        load.wait()
    wqv_t[0:width] = w_qkv[:, :width].astype(F32).T.astype(BF16)
    wqv_t[width:] = w_qkv[:, 2 * width :].astype(F32).T.astype(BF16)

    def attention(row, carry):
        settle(got, recv_sems, 0, row)
        base = unpack(got[row].astype(F32), feats, width, packed)
        normed = cell_norm(base, gain_one[...])
        context = attend(normed, w_qkv[:, width : 2 * width], wqv_t[...])
        sent = pack(context.reshape(n, feats, width), packed).astype(BF16)
        ctx[row] = sent
        spread(ctx, back, 1, row)
        back[row, pl.ds(me, 1)] = ctx[row, pl.ds(me, 1)]
        return carry

    lax.fori_loop(0, rows, attention, 0)

    def store(row):
        return pltpu.make_async_copy(done.at[row], out.at[:, row], out_sems.at[row])

    def finish(row, carry):
        settle(back, recv_sems, 1, row)
        context = unpack(back[row].astype(F32), feats, width, packed).astype(BF16)
        base = unpack(tok[row].astype(F32), feats, width, packed)
        mid = base + jnp.dot(context, w_out[...], preferred_element_type=F32)
        normed = cell_norm(mid, gain_two[...])
        hidden = jnp.dot(normed, w_up[...], preferred_element_type=F32)
        act = (0.5 * hidden * (1.0 + lax.erf(hidden * math.sqrt(0.5)))).astype(BF16)
        result = mid + lax.dot_general(
            act, w_down[...], (((1,), (1,)), ((), ())), preferred_element_type=F32
        )
        done[row] = result.reshape(n, feats, width)
        store(row).start()
        return carry

    lax.fori_loop(0, rows, finish, 0)

    for row in range(rows):
        settle(tok, send_sems, 0, row)
        settle(ctx, send_sems, 1, row)
        store(row).wait()


def body(
    cells, missing, feat_ids, feat_table, nan_embed, gain_one, w_qkv, w_out, gain_two, w_up, w_down
):
    n = lax.axis_size("feat")
    all_rows, feats, width = cells.shape
    rows = all_rows // n
    packed = width == 192 and feats % 32 == 0
    piece = (feats + feats // 2, 128) if packed else (feats, width)
    buffer = pltpu.VMEM((rows, n) + piece, BF16)
    operands = (
        cells.reshape(n, rows, feats, width),
        missing.T,
        feat_ids[None],
        feat_table,
        nan_embed[None],
        gain_one[None],
        w_qkv,
        w_out,
        gain_two[None],
        w_up,
        w_down.T,
    )
    result = pl.pallas_call(
        functools.partial(kernel, n, rows, feats, width, packed),
        out_shape=pltpu.VMEM((n, rows, feats, width), F32),
        in_specs=[pl.BlockSpec(memory_space=pltpu.HBM)] * len(operands),
        out_specs=pl.BlockSpec(memory_space=pltpu.VMEM),
        scratch_shapes=[pltpu.VMEM(x.shape, x.dtype) for x in operands]
        + [
            buffer,
            buffer,
            buffer,
            buffer,
            pltpu.VMEM((2 * width, width), BF16),
            pltpu.VMEM((rows, n, feats, width), F32),
            pltpu.SemaphoreType.DMA((len(operands),)),
            pltpu.SemaphoreType.DMA((2, rows)),
            pltpu.SemaphoreType.DMA((2, rows)),
            pltpu.SemaphoreType.DMA((rows,)),
        ],
        compiler_params=pltpu.CompilerParams(
            collective_id=0, has_side_effects=True, vmem_limit_bytes=LIMIT
        ),
    )(*operands)
    return result.reshape(all_rows, feats, width)


def solution(mesh):
    in_specs = (
        P("groups", "feat", None),
        P("groups", "feat"),
        P(("groups", "feat")),
        P(),
        P(),
        P(),
        P(),
        P(),
        P(),
        P(),
        P(),
    )
    out_specs = P("groups", "feat", None)
    return jax.shard_map(body, mesh=mesh, in_specs=in_specs, out_specs=out_specs, check_vma=False)
```

```python
import functools
import math

import jax
import jax.numpy as jnp
from jax import lax
from jax.experimental import pallas as pl
from jax.experimental.pallas import tpu as pltpu
from jax.sharding import PartitionSpec as P

HEADS = 6
MESH = pl.DeviceIdType.MESH
F32 = jnp.float32
BF16 = jnp.bfloat16
LIMIT = 58 * 1024 * 1024


def cell_norm(values, gain):
    mean = jnp.mean(values, axis=-1, keepdims=True)
    centered = values - mean
    var = jnp.mean(centered * centered, axis=-1, keepdims=True)
    return (centered * lax.rsqrt(var + 1e-05) * gain).astype(BF16)


def pack(values, packed):
    if not packed:
        return values
    half = values.shape[-2] // 2
    tail = values[..., 128:]
    tail = jnp.concatenate([tail[..., :half, :], tail[..., half:, :]], axis=-1)
    return jnp.concatenate([values[..., :128], tail], axis=-2)


def unpack(values, feats, width, packed):
    if packed:
        rest = width - 128
        tail = values[:, feats:]
        tail = jnp.concatenate([tail[..., :rest], tail[..., rest:]], axis=-2)
        values = jnp.concatenate([values[:, :feats], tail], axis=-1)
    return values.reshape(values.shape[0] * feats, width)


def lanes(head, head_dim, width):
    low = head * head_dim
    block = low // 128 * 128
    return low, block, min(block + 128, width)


def project(normed, wk, wqv_t, keys, query, value, first, count):
    width = wk.shape[0]
    head_dim = width // HEADS
    here = slice(first, first + count)
    keys[here] = jnp.dot(normed, wk, preferred_element_type=F32).astype(BF16)
    turned = lax.dot_general(
        wqv_t, normed, (((1,), (1,)), ((), ())), preferred_element_type=F32
    ).astype(BF16)
    for head in range(HEADS):
        low, block, high = lanes(head, head_dim, width)
        query[head, low - block : low - block + head_dim, here] = turned[low : low + head_dim]
        value[head, 0:head_dim, here] = turned[width + low : width + low + head_dim]


def score(keys, query, head, width):
    _, block, high = lanes(head, width // HEADS, width)
    return jnp.dot(
        keys[:, block:high], query[head, 0 : high - block], preferred_element_type=F32
    )


def weigh(scores, value, head, head_dim):
    scale = head_dim ** (-0.5) * math.log2(math.e)
    top = jnp.max(scores, axis=0, keepdims=True)
    expo = jnp.exp2((scores - top) * scale).astype(BF16)
    sums = jnp.dot(value[head], expo, preferred_element_type=F32)
    return sums[:head_dim] / sums[head_dim : head_dim + 1]


def feed(context, base, w_out, gain_two, w_up, w_down, feats, width, packed):
    context = unpack(context.astype(F32), feats, width, packed).astype(BF16)
    base = unpack(base.astype(F32), feats, width, packed)
    mid = base + jnp.dot(context, w_out[...], preferred_element_type=F32)
    normed = cell_norm(mid, gain_two[...])
    hidden = jnp.dot(normed, w_up[...], preferred_element_type=F32)
    act = (0.5 * hidden * (1.0 + lax.erf(hidden * math.sqrt(0.5)))).astype(BF16)
    return mid + lax.dot_general(
        act, w_down[...], (((1,), (1,)), ((), ())), preferred_element_type=F32
    )


def close(n, rows, feats, width, packed, *refs):
    done, back, tok, w_out, gain_two, w_up, w_down, out, last, sems = refs
    half = n // 2
    mine = lax.axis_index("feat") // half * half
    other = half - mine
    final = rows - 1
    copies = [
        pltpu.make_async_copy(done.at[row], out.at[:, row], sems.at[row]) for row in range(final)
    ]
    here = pl.ds(mine, half)
    copies.append(pltpu.make_async_copy(done.at[final, here], out.at[here, final], sems.at[final]))
    for copy in copies:
        copy.start()
    here = pl.ds(other, half)
    last[...] = feed(
        back[final, here], tok[final, here], w_out, gain_two, w_up, w_down, feats, width, packed
    ).reshape(half, feats, width)
    copies.append(pltpu.make_async_copy(last, out.at[here, final], sems.at[rows]))
    copies[-1].start()
    for copy in copies:
        copy.wait()


def kernel(n, rows, feats, width, packed, *refs):
    sources, refs = refs[:11], refs[11:]
    done, back, tok, w_out, gain_two, w_up, w_down = refs[:7]
    held, refs = refs[7:14] + (w_out, gain_two, w_up, w_down), refs[14:]
    got, ctx, wqv_t, keys, query, value, turned, even, odd, load_sems, cell_sems, send_sems, recv_sems, all_sem = refs
    (cells, missing, feat_ids, feat_table, nan_embed) = held[:5]
    gain_one, w_qkv = held[5:7]
    scores = (even, odd)
    me = lax.axis_index("feat")
    half = n // 2
    quarter = half // 2
    mine = me // half * half
    other = half - mine
    high = me >= half
    barrier = pltpu.get_barrier_semaphore()

    def greet(peer):
        pl.semaphore_signal(barrier, inc=1, device_id={"feat": peer}, device_id_type=MESH)

    def greet_other(step, carry):
        greet(other + step)
        return carry

    def greet_mine(step, carry):
        greet(mine + lax.rem(me - mine + step, half))
        return carry

    def greet_near():
        lax.fori_loop(1, half, greet_mine, 0)

    lax.fori_loop(0, half, greet_other, 0)
    pl.when(jnp.logical_not(high))(greet_near)

    cell_loads = [
        pltpu.make_async_copy(sources[0].at[:, row], cells.at[:, row], cell_sems.at[row])
        for row in range(rows)
    ]
    loads = [
        pltpu.make_async_copy(source, target, load_sems.at[spot])
        for spot, (source, target) in enumerate(zip(sources[1:], held[1:]))
    ]
    for load in loads[:4] + cell_loads[:1] + loads[4:5] + cell_loads[1:] + loads[5:]:
        load.start()
    for load in loads[:4]:
        load.wait()

    ncat = feat_table.shape[0]
    hot = (lax.broadcasted_iota(jnp.int32, (ncat, feats), 0) == feat_ids[...]).astype(F32)
    femb = lax.dot_general(
        hot, feat_table[...], (((0,), (0,)), ((), ())),
        precision=lax.Precision.HIGHEST, preferred_element_type=F32,
    )
    nan = nan_embed[...]
    absent = missing[...].astype(F32)

    def give(source, target, kind, row, side, peer):
        pltpu.make_async_remote_copy(
            src_ref=source.at[row, peer],
            dst_ref=target.at[row, me],
            send_sem=send_sems.at[kind, row],
            recv_sem=recv_sems.at[kind, row, side],
            device_id={"feat": peer},
            device_id_type=MESH,
        ).start()

    def spread(source, target, kind, row):
        def one(step, carry):
            peer = me + step
            peer = jnp.where(peer < n, peer, peer - n)
            side = jnp.where((peer >= mine) & (peer < mine + half), 0, 1)
            give(source, target, kind, row, side, peer)
            return carry

        lax.fori_loop(1, n, one, 0)

    def settle(ref, sem, row, count):
        piece = ref.at[row, pl.ds(0, count)]
        pltpu.make_async_copy(piece, piece, sem).wait()

    def arrive(ref, kind, row, side):
        settle(ref, recv_sems.at[kind, row, side], row, half - 1 + side)

    def build(row, peer):
        spot = peer * rows + row
        values = cells[peer, row].astype(F32)
        values = (values + absent[:, spot : spot + 1] * nan + femb).astype(BF16)
        tok[row, peer] = pack(values, packed)

    def open_high():
        pl.semaphore_wait(barrier, half)

    cell_loads[0].wait()
    pl.when(high)(open_high)
    for peer in range(n):
        build(0, peer)
        if peer < half:
            pl.when(high)(lambda peer=peer: give(tok, got, 0, 0, 1, peer))
    for row in range(1, rows):
        cell_loads[row].wait()
        for peer in range(n):
            build(row, peer)

    def near(step, carry):
        give(tok, got, 0, 0, 0, mine + lax.rem(me - mine + step, half))
        return carry

    def open_low():
        pl.semaphore_wait(barrier, n - 1)

    def tell(ahead):
        pl.semaphore_signal(
            all_sem, inc=1, device_id={"feat": me + ahead}, device_id_type=MESH
        )

    def tell_high():
        tell(quarter)
        tell(half)

    def first_low():
        spread(tok, got, 0, 0)

    def first_high():
        pl.semaphore_wait(all_sem, 1)
        lax.fori_loop(1, half, near, 0)

    low = jnp.logical_not(high)
    pl.when(low)(open_low)
    pl.when(low & (me >= half - quarter))(tell_high)
    pl.when(low)(first_low)
    pl.when(high)(first_high)
    for row in range(1, rows):
        spread(tok, got, 0, row)
    for row in range(rows):
        got[row, pl.ds(me, 1)] = tok[row, pl.ds(me, 1)]
    for load in loads[4:]:
        load.wait()
    gain = gain_one[...]
    wqv_t[0:width] = w_qkv[:, :width].astype(F32).T.astype(BF16)
    wqv_t[width:] = w_qkv[:, 2 * width :].astype(F32).T.astype(BF16)

    head_dim = width // HEADS
    count = n * feats
    query[...] = jnp.zeros_like(query)
    value[...] = jnp.ones_like(value)

    def attention(row, carry):
        arrive(got, 0, row, 0)
        arrive(got, 0, row, 1)
        normed = cell_norm(unpack(got[row].astype(F32), feats, width, packed), gain)
        project(normed, w_qkv[:, width : 2 * width], wqv_t[...], keys, query, value, 0, count)
        scores[0][...] = score(keys, query, 0, width)
        for head in range(HEADS):
            if head + 1 < HEADS:
                scores[(head + 1) % 2][...] = score(keys, query, head + 1, width)
            turned[head * head_dim : (head + 1) * head_dim] = weigh(
                scores[head % 2][...], value, head, head_dim
            )
        context = turned[...].T
        ctx[row] = pack(context.reshape(n, feats, width), packed).astype(BF16)
        spread(ctx, back, 1, row)
        back[row, pl.ds(me, 1)] = ctx[row, pl.ds(me, 1)]
        return carry

    lax.fori_loop(0, rows, attention, 0)

    def finish(row, first, count):
        here = pl.ds(first, count)
        done[row, here] = feed(
            back[row, here], tok[row, here], w_out, gain_two, w_up, w_down, feats, width, packed
        ).reshape(count, feats, width)

    def whole(row, carry):
        arrive(back, 1, row, 0)
        arrive(back, 1, row, 1)
        finish(row, 0, n)
        return carry

    lax.fori_loop(0, rows - 1, whole, 0)
    arrive(back, 1, rows - 1, 0)
    finish(rows - 1, mine, half)
    arrive(back, 1, rows - 1, 1)
    for row in range(rows):
        settle(tok, send_sems.at[0, row], row, n - 1)
        settle(ctx, send_sems.at[1, row], row, n - 1)


def body(
    cells, missing, feat_ids, feat_table, nan_embed, gain_one, w_qkv, w_out, gain_two, w_up, w_down
):
    n = lax.axis_size("feat")
    all_rows, feats, width = cells.shape
    rows = all_rows // n
    packed = width == 192 and feats % 32 == 0
    piece = (feats + feats // 2, 128) if packed else (feats, width)
    buffer = pltpu.VMEM((rows, n) + piece, BF16)
    operands = (
        cells.reshape(n, rows, feats, width),
        missing.T,
        feat_ids[None],
        feat_table,
        nan_embed[None],
        gain_one[None],
        w_qkv,
        w_out,
        gain_two[None],
        w_up,
        w_down.T,
    )
    kept = pltpu.VMEM((rows, n) + piece, BF16)
    results = pl.pallas_call(
        functools.partial(kernel, n, rows, feats, width, packed),
        out_shape=[pltpu.VMEM((rows, n, feats, width), F32), kept, kept]
        + [pltpu.VMEM(x.shape, x.dtype) for x in operands[7:]],
        in_specs=[pl.BlockSpec(memory_space=pltpu.HBM)] * len(operands),
        out_specs=[pl.BlockSpec(memory_space=pltpu.VMEM)] * 7,
        scratch_shapes=[pltpu.VMEM(x.shape, x.dtype) for x in operands[:7]]
        + [
            buffer,
            buffer,
            pltpu.VMEM((2 * width, width), BF16),
            pltpu.VMEM((n * feats, width), BF16),
            pltpu.VMEM((HEADS, 128, n * feats), BF16),
            pltpu.VMEM((HEADS, width // HEADS + 16, n * feats), BF16),
            pltpu.VMEM((width, n * feats), F32),
            pltpu.VMEM((n * feats, n * feats), F32),
            pltpu.VMEM((n * feats, n * feats), F32),
            pltpu.SemaphoreType.DMA((len(operands) - 1,)),
            pltpu.SemaphoreType.DMA((rows,)),
            pltpu.SemaphoreType.DMA((2, rows)),
            pltpu.SemaphoreType.DMA((2, rows, 2)),
            pltpu.SemaphoreType.REGULAR,
        ],
        compiler_params=pltpu.CompilerParams(
            collective_id=0, has_side_effects=True, vmem_limit_bytes=LIMIT
        ),
    )(*operands)
    result = pl.pallas_call(
        functools.partial(close, n, rows, feats, width, packed),
        out_shape=jax.ShapeDtypeStruct((n, rows, feats, width), F32),
        in_specs=[pl.BlockSpec(memory_space=pltpu.VMEM)] * 7,
        out_specs=pl.BlockSpec(memory_space=pltpu.HBM),
        scratch_shapes=[
            pltpu.VMEM((n // 2, feats, width), F32),
            pltpu.SemaphoreType.DMA((rows + 1,)),
        ],
        compiler_params=pltpu.CompilerParams(vmem_limit_bytes=8 * 1024 * 1024),
    )(*results)
    return result.reshape(all_rows, feats, width)


def solution(mesh):
    in_specs = (
        P("groups", "feat", None),
        P("groups", "feat"),
        P(("groups", "feat")),
        P(),
        P(),
        P(),
        P(),
        P(),
        P(),
        P(),
        P(),
    )
    out_specs = P("groups", "feat", None)
    return jax.shard_map(body, mesh=mesh, in_specs=in_specs, out_specs=out_specs, check_vma=False)
```

```python
import functools
import math

import jax
import jax.numpy as jnp
from jax import lax
from jax.experimental import pallas as pl
from jax.experimental.pallas import tpu as pltpu
from jax.sharding import PartitionSpec as P

HEADS = 6
MESH = pl.DeviceIdType.MESH
F32 = jnp.float32
BF16 = jnp.bfloat16
LIMIT = 58 * 1024 * 1024


def cell_norm(values, gain):
    mean = jnp.mean(values, axis=-1, keepdims=True)
    centered = values - mean
    var = jnp.mean(centered * centered, axis=-1, keepdims=True)
    return (centered * lax.rsqrt(var + 1e-05) * gain).astype(BF16)


def pack(values, packed):
    if not packed:
        return values
    half = values.shape[-2] // 2
    tail = values[..., 128:]
    tail = jnp.concatenate([tail[..., :half, :], tail[..., half:, :]], axis=-1)
    return jnp.concatenate([values[..., :128], tail], axis=-2)


def unpack(values, feats, width, packed):
    if packed:
        rest = width - 128
        tail = values[:, feats:]
        tail = jnp.concatenate([tail[..., :rest], tail[..., rest:]], axis=-2)
        values = jnp.concatenate([values[:, :feats], tail], axis=-1)
    return values.reshape(values.shape[0] * feats, width)


def lanes(head, head_dim, width):
    low = head * head_dim
    block = low // 128 * 128
    return low, block, min(block + 128, width)


def project(normed, wk, wqv_t, keys, query, value, first, count):
    width = wk.shape[0]
    head_dim = width // HEADS
    here = slice(first, first + count)
    keys[here] = jnp.dot(normed, wk, preferred_element_type=F32).astype(BF16)
    turned = lax.dot_general(
        wqv_t, normed, (((1,), (1,)), ((), ())), preferred_element_type=F32
    ).astype(BF16)
    for head in range(HEADS):
        low, block, high = lanes(head, head_dim, width)
        query[head, low - block : low - block + head_dim, here] = turned[low : low + head_dim]
        value[head, 0:head_dim, here] = turned[width + low : width + low + head_dim]


def score(keys, query, head, width):
    _, block, high = lanes(head, width // HEADS, width)
    return jnp.dot(
        keys[:, block:high], query[head, 0 : high - block], preferred_element_type=F32
    )


def weigh(scores, value, head, head_dim):
    scale = head_dim ** (-0.5) * math.log2(math.e)
    top = jnp.max(scores, axis=0, keepdims=True)
    expo = jnp.exp2((scores - top) * scale).astype(BF16)
    sums = jnp.dot(value[head], expo, preferred_element_type=F32)
    return sums[:head_dim] / sums[head_dim : head_dim + 1]


def feed(context, base, w_out, gain_two, w_up, w_down, feats, width, packed):
    context = unpack(context.astype(F32), feats, width, packed).astype(BF16)
    base = unpack(base.astype(F32), feats, width, packed)
    mid = base + jnp.dot(context, w_out[...], preferred_element_type=F32)
    normed = cell_norm(mid, gain_two[...])
    hidden = jnp.dot(normed, w_up[...], preferred_element_type=F32)
    act = (0.5 * hidden * (1.0 + lax.erf(hidden * math.sqrt(0.5)))).astype(BF16)
    return mid + lax.dot_general(
        act, w_down[...], (((1,), (1,)), ((), ())), preferred_element_type=F32
    )


def close(n, rows, feats, width, packed, *refs):
    done, back, tok, w_out, gain_two, w_up, w_down, out, last, sems = refs
    half = n // 2
    quarter = half // 2
    me = lax.axis_index("feat")
    mine = me // half * half
    other = half - mine
    inner_high = me // quarter == 2
    final = rows - 1
    copies = [
        pltpu.make_async_copy(done.at[row], out.at[:, row], sems.at[row]) for row in range(final)
    ]
    here = pl.ds(jnp.where(inner_high, other, mine), half)
    copies.append(pltpu.make_async_copy(done.at[final, here], out.at[here, final], sems.at[final]))
    for copy in copies:
        copy.start()
    here = pl.ds(jnp.where(inner_high, mine, other), half)
    last[...] = feed(
        back[final, here], tok[final, here], w_out, gain_two, w_up, w_down, feats, width, packed
    ).reshape(half, feats, width)
    copies.append(pltpu.make_async_copy(last, out.at[here, final], sems.at[rows]))
    copies[-1].start()
    for copy in copies:
        copy.wait()


def kernel(n, rows, feats, width, packed, *refs):
    sources, refs = refs[:11], refs[11:]
    done, back, tok, w_out, gain_two, w_up, w_down = refs[:7]
    held, refs = refs[7:14] + (w_out, gain_two, w_up, w_down), refs[14:]
    got, ctx, wqv_t, keys, query, value, turned, even, odd, load_sems, cell_sems, send_sems, recv_sems, all_sem = refs
    (cells, missing, feat_ids, feat_table, nan_embed) = held[:5]
    gain_one, w_qkv = held[5:7]
    scores = (even, odd)
    me = lax.axis_index("feat")
    half = n // 2
    quarter = half // 2
    mine = me // half * half
    other = half - mine
    high = me >= half
    barrier = pltpu.get_barrier_semaphore()

    part = me // quarter
    inner_low = part == 1
    inner_high = part == 2
    outer = (part == 0) | (part == 3)

    def greet(first, skip):
        def one(step, carry):
            peer = first + lax.rem(me - part * quarter + step, quarter)
            pl.semaphore_signal(barrier, inc=1, device_id={"feat": peer}, device_id_type=MESH)
            return carry

        lax.fori_loop(skip, quarter, one, 0)

    pl.when(me < half)(lambda: greet(half, 0))
    pl.when(inner_high)(lambda: greet(quarter, 0))
    greet(0, jnp.where(part == 0, 1, 0))
    greet(half + quarter, jnp.where(part == 3, 1, 0))

    cell_loads = [
        pltpu.make_async_copy(sources[0].at[:, row], cells.at[:, row], cell_sems.at[row])
        for row in range(rows)
    ]
    loads = [
        pltpu.make_async_copy(source, target, load_sems.at[spot])
        for spot, (source, target) in enumerate(zip(sources[1:], held[1:]))
    ]
    for load in loads[:4] + cell_loads[:1] + loads[4:5] + cell_loads[1:] + loads[5:]:
        load.start()
    for load in loads[:4]:
        load.wait()

    ncat = feat_table.shape[0]
    hot = (lax.broadcasted_iota(jnp.int32, (ncat, feats), 0) == feat_ids[...]).astype(F32)
    femb = lax.dot_general(
        hot, feat_table[...], (((0,), (0,)), ((), ())),
        precision=lax.Precision.HIGHEST, preferred_element_type=F32,
    )
    nan = nan_embed[...]
    absent = missing[...].astype(F32)

    def give(source, target, kind, row, side, peer):
        pltpu.make_async_remote_copy(
            src_ref=source.at[row, peer],
            dst_ref=target.at[row, me],
            send_sem=send_sems.at[kind, row],
            recv_sem=recv_sems.at[kind, row, side],
            device_id={"feat": peer},
            device_id_type=MESH,
        ).start()

    def spread(source, target, kind, row):
        def one(step, carry):
            peer = me + step
            peer = jnp.where(peer < n, peer, peer - n)
            side = jnp.where((peer >= mine) & (peer < mine + half), 0, 1)
            give(source, target, kind, row, side, peer)
            return carry

        lax.fori_loop(1, n, one, 0)

    def settle(ref, sem, row, count):
        piece = ref.at[row, pl.ds(0, count)]
        pltpu.make_async_copy(piece, piece, sem).wait()

    def arrive(ref, kind, row, side):
        settle(ref, recv_sems.at[kind, row, side], row, half - 1 + side)

    def build(row, peer):
        spot = peer * rows + row
        values = cells[peer, row].astype(F32)
        values = (values + absent[:, spot : spot + 1] * nan + femb).astype(BF16)
        tok[row, peer] = pack(values, packed)

    def tell(ahead):
        pl.semaphore_signal(
            all_sem, inc=1, device_id={"feat": me - ahead}, device_id_type=MESH
        )

    def open_outer():
        pl.semaphore_wait(barrier, n - 1)

    def tell_inner():
        tell(quarter)
        tell(half)

    def open_high():
        pl.semaphore_wait(barrier, half)

    def open_low():
        pl.semaphore_wait(barrier, quarter)
        lax.fori_loop(0, quarter, across, 0)

    def across(step, carry):
        give(tok, got, 0, 0, 1, half + lax.rem(me + step, quarter))
        return carry

    def beyond(step, carry):
        give(tok, got, 0, 0, 1, half + quarter + lax.rem(me + step, quarter))
        return carry

    def near(step, carry):
        give(tok, got, 0, 0, 0, mine + lax.rem(me - mine + step, half))
        return carry

    def wait_all():
        pl.semaphore_wait(all_sem, 1)

    def open_last():
        open_outer()
        tell_inner()

    cell_loads[0].wait()
    pl.when(part == 3)(open_last)
    pl.when(inner_high)(open_high)
    for peer in range(n):
        build(0, peer)
        if peer < half:
            pl.when(high)(lambda peer=peer: give(tok, got, 0, 0, 1, peer))
    pl.when(inner_low)(open_low)
    for row in range(1, rows):
        cell_loads[row].wait()
        for peer in range(n):
            build(row, peer)
    pl.when(part == 0)(open_outer)
    pl.when(inner_low | inner_high)(wait_all)

    def first_low():
        spread(tok, got, 0, 0)

    def first_rest():
        lax.fori_loop(1, half, near, 0)

    def first_beyond():
        lax.fori_loop(0, quarter, beyond, 0)

    pl.when(part == 0)(first_low)
    pl.when(part > 0)(first_rest)
    pl.when(inner_low)(first_beyond)
    for row in range(1, rows):
        spread(tok, got, 0, row)
    for row in range(rows):
        got[row, pl.ds(me, 1)] = tok[row, pl.ds(me, 1)]
    for load in loads[4:]:
        load.wait()
    gain = gain_one[...]
    wqv_t[0:width] = w_qkv[:, :width].astype(F32).T.astype(BF16)
    wqv_t[width:] = w_qkv[:, 2 * width :].astype(F32).T.astype(BF16)

    head_dim = width // HEADS
    count = n * feats
    query[...] = jnp.zeros_like(query)
    value[...] = jnp.ones_like(value)

    def attention(row, carry):
        arrive(got, 0, row, 0)
        arrive(got, 0, row, 1)
        normed = cell_norm(unpack(got[row].astype(F32), feats, width, packed), gain)
        project(normed, w_qkv[:, width : 2 * width], wqv_t[...], keys, query, value, 0, count)
        scores[0][...] = score(keys, query, 0, width)
        for head in range(HEADS):
            if head + 1 < HEADS:
                scores[(head + 1) % 2][...] = score(keys, query, head + 1, width)
            turned[head * head_dim : (head + 1) * head_dim] = weigh(
                scores[head % 2][...], value, head, head_dim
            )
        context = turned[...].T
        ctx[row] = pack(context.reshape(n, feats, width), packed).astype(BF16)
        spread(ctx, back, 1, row)
        pltpu.make_async_copy(
            ctx.at[row, me], back.at[row, me], recv_sems.at[1, row, 0]
        ).start()
        return carry

    lax.fori_loop(0, rows, attention, 0)

    before = max(rows - 1, 1)

    def finish(step, carry):
        row = jnp.where(inner_high, step // 2, step % rows)
        side = jnp.where(inner_high, 1 - step % 2, step // rows)
        row = jnp.where(part == 0, jnp.where(step < 2 * before, step % before, rows - 1), row)
        side = jnp.where(part == 0, step // before % 2, side)
        settle(back, recv_sems.at[1, row, side], row, half)
        here = pl.ds(jnp.where(side == 0, mine, other), half)
        done[row, here] = feed(
            back[row, here], tok[row, here], w_out, gain_two, w_up, w_down, feats, width, packed
        ).reshape(half, feats, width)
        return carry

    lax.fori_loop(0, 2 * rows - 1, finish, 0)
    settle(back, recv_sems.at[1, rows - 1, jnp.where(inner_high, 0, 1)], rows - 1, half)

    for row in range(rows):
        settle(tok, send_sems.at[0, row], row, n - 1)
        settle(ctx, send_sems.at[1, row], row, n - 1)


def body(
    cells, missing, feat_ids, feat_table, nan_embed, gain_one, w_qkv, w_out, gain_two, w_up, w_down
):
    n = lax.axis_size("feat")
    all_rows, feats, width = cells.shape
    rows = all_rows // n
    packed = width == 192 and feats % 32 == 0
    piece = (feats + feats // 2, 128) if packed else (feats, width)
    buffer = pltpu.VMEM((rows, n) + piece, BF16)
    operands = (
        cells.reshape(n, rows, feats, width),
        missing.T,
        feat_ids[None],
        feat_table,
        nan_embed[None],
        gain_one[None],
        w_qkv,
        w_out,
        gain_two[None],
        w_up,
        w_down.T,
    )
    kept = pltpu.VMEM((rows, n) + piece, BF16)
    results = pl.pallas_call(
        functools.partial(kernel, n, rows, feats, width, packed),
        out_shape=[pltpu.VMEM((rows, n, feats, width), F32), kept, kept]
        + [pltpu.VMEM(x.shape, x.dtype) for x in operands[7:]],
        in_specs=[pl.BlockSpec(memory_space=pltpu.HBM)] * len(operands),
        out_specs=[pl.BlockSpec(memory_space=pltpu.VMEM)] * 7,
        scratch_shapes=[pltpu.VMEM(x.shape, x.dtype) for x in operands[:7]]
        + [
            buffer,
            buffer,
            pltpu.VMEM((2 * width, width), BF16),
            pltpu.VMEM((n * feats, width), BF16),
            pltpu.VMEM((HEADS, 128, n * feats), BF16),
            pltpu.VMEM((HEADS, width // HEADS + 16, n * feats), BF16),
            pltpu.VMEM((width, n * feats), F32),
            pltpu.VMEM((n * feats, n * feats), F32),
            pltpu.VMEM((n * feats, n * feats), F32),
            pltpu.SemaphoreType.DMA((len(operands) - 1,)),
            pltpu.SemaphoreType.DMA((rows,)),
            pltpu.SemaphoreType.DMA((2, rows)),
            pltpu.SemaphoreType.DMA((2, rows, 2)),
            pltpu.SemaphoreType.REGULAR,
        ],
        compiler_params=pltpu.CompilerParams(
            collective_id=0, has_side_effects=True, vmem_limit_bytes=LIMIT
        ),
    )(*operands)
    result = pl.pallas_call(
        functools.partial(close, n, rows, feats, width, packed),
        out_shape=jax.ShapeDtypeStruct((n, rows, feats, width), F32),
        in_specs=[pl.BlockSpec(memory_space=pltpu.VMEM)] * 7,
        out_specs=pl.BlockSpec(memory_space=pltpu.HBM),
        scratch_shapes=[
            pltpu.VMEM((n // 2, feats, width), F32),
            pltpu.SemaphoreType.DMA((rows + 1,)),
        ],
        compiler_params=pltpu.CompilerParams(vmem_limit_bytes=8 * 1024 * 1024),
    )(*results)
    return result.reshape(all_rows, feats, width)


def solution(mesh):
    in_specs = (
        P("groups", "feat", None),
        P("groups", "feat"),
        P(("groups", "feat")),
        P(),
        P(),
        P(),
        P(),
        P(),
        P(),
        P(),
        P(),
    )
    out_specs = P("groups", "feat", None)
    return jax.shard_map(body, mesh=mesh, in_specs=in_specs, out_specs=out_specs, check_vma=False)
```

```python
import functools
import math

import jax
import jax.numpy as jnp
from jax import lax
from jax.experimental import pallas as pl
from jax.experimental.pallas import tpu as pltpu
from jax.sharding import PartitionSpec as P

HEADS = 6
MESH = pl.DeviceIdType.MESH
F32 = jnp.float32
BF16 = jnp.bfloat16
LIMIT = 58 * 1024 * 1024


def cell_norm(values, gain):
    mean = jnp.mean(values, axis=-1, keepdims=True)
    centered = values - mean
    var = jnp.mean(centered * centered, axis=-1, keepdims=True)
    return (centered * lax.rsqrt(var + 1e-05) * gain).astype(BF16)


def pack(values, packed):
    if not packed:
        return values
    half = values.shape[-2] // 2
    tail = values[..., 128:]
    tail = jnp.concatenate([tail[..., :half, :], tail[..., half:, :]], axis=-1)
    return jnp.concatenate([values[..., :128], tail], axis=-2)


def unpack(values, feats, width, packed):
    if packed:
        rest = width - 128
        tail = values[:, feats:]
        tail = jnp.concatenate([tail[..., :rest], tail[..., rest:]], axis=-2)
        values = jnp.concatenate([values[:, :feats], tail], axis=-1)
    return values.reshape(values.shape[0] * feats, width)


def lanes(head, head_dim, width):
    low = head * head_dim
    block = low // 128 * 128
    return low, block, min(block + 128, width)


def project(normed, wk, wqv_t, keys, query, value, first, count):
    width = wk.shape[0]
    head_dim = width // HEADS
    here = slice(first, first + count)
    keys[here] = jnp.dot(normed, wk, preferred_element_type=F32).astype(BF16)
    turned = lax.dot_general(
        wqv_t, normed, (((1,), (1,)), ((), ())), preferred_element_type=F32
    ).astype(BF16)
    for head in range(HEADS):
        low, block, high = lanes(head, head_dim, width)
        query[head, low - block : low - block + head_dim, here] = turned[low : low + head_dim]
        value[head, 0:head_dim, here] = turned[width + low : width + low + head_dim]


def score(keys, query, head, width):
    _, block, high = lanes(head, width // HEADS, width)
    return jnp.dot(
        keys[:, block:high], query[head, 0 : high - block], preferred_element_type=F32
    )


def weigh(scores, value, head, head_dim):
    scale = head_dim ** (-0.5) * math.log2(math.e)
    top = jnp.max(scores, axis=0, keepdims=True)
    expo = jnp.exp2((scores - top) * scale).astype(BF16)
    sums = jnp.dot(value[head], expo, preferred_element_type=F32)
    return sums[:head_dim] / sums[head_dim : head_dim + 1]


def feed(context, base, w_out, gain_two, w_up, w_down, feats, width, packed):
    context = unpack(context.astype(F32), feats, width, packed).astype(BF16)
    base = unpack(base.astype(F32), feats, width, packed)
    mid = base + jnp.dot(context, w_out[...], preferred_element_type=F32)
    normed = cell_norm(mid, gain_two[...])
    hidden = jnp.dot(normed, w_up[...], preferred_element_type=F32)
    act = (0.5 * hidden * (1.0 + lax.erf(hidden * math.sqrt(0.5)))).astype(BF16)
    return mid + lax.dot_general(
        act, w_down[...], (((1,), (1,)), ((), ())), preferred_element_type=F32
    )


def close(n, rows, feats, width, packed, *refs):
    done, back, tok, w_out, gain_two, w_up, w_down, out, last, sems = refs
    half = n // 2
    mine = lax.axis_index("feat") // half * half
    other = half - mine
    final = rows - 1
    copies = [
        pltpu.make_async_copy(done.at[row], out.at[:, row], sems.at[row]) for row in range(final)
    ]
    here = pl.ds(mine, half)
    copies.append(pltpu.make_async_copy(done.at[final, here], out.at[here, final], sems.at[final]))
    for copy in copies:
        copy.start()
    here = pl.ds(other, half)
    last[...] = feed(
        back[final, here], tok[final, here], w_out, gain_two, w_up, w_down, feats, width, packed
    ).reshape(half, feats, width)
    copies.append(pltpu.make_async_copy(last, out.at[here, final], sems.at[rows]))
    copies[-1].start()
    for copy in copies:
        copy.wait()


def kernel(n, rows, feats, width, packed, *refs):
    sources, refs = refs[:11], refs[11:]
    done, back, tok, w_out, gain_two, w_up, w_down = refs[:7]
    held, refs = refs[7:14] + (w_out, gain_two, w_up, w_down), refs[14:]
    got, ctx, wqv_t, keys, query, value, turned, even, odd = refs[:9]
    load_sems, cell_sems, send_sems, recv_sems, all_sem = refs[9:]
    (cells, missing, feat_ids, feat_table, nan_embed) = held[:5]
    gain_one, w_qkv = held[5:7]
    scores = (even, odd)
    me = lax.axis_index("feat")
    half = n // 2
    quarter = half // 2
    mine = me // half * half
    other = half - mine
    high = me >= half
    barrier = pltpu.get_barrier_semaphore()

    part = me // quarter
    inner_low = part == 1
    inner_high = part == 2
    outer = (part == 0) | (part == 3)

    def greet(first, skip):
        def one(step, carry):
            peer = first + lax.rem(me - part * quarter + step, quarter)
            pl.semaphore_signal(barrier, inc=1, device_id={"feat": peer}, device_id_type=MESH)
            return carry

        lax.fori_loop(skip, quarter, one, 0)

    pl.when(me < half)(lambda: greet(half, 0))
    pl.when(inner_high)(lambda: greet(quarter, 0))
    greet(0, jnp.where(part == 0, 1, 0))
    greet(half + quarter, jnp.where(part == 3, 1, 0))

    cell_loads = [
        pltpu.make_async_copy(sources[0].at[:, row], cells.at[:, row], cell_sems.at[row])
        for row in range(rows)
    ]
    loads = [
        pltpu.make_async_copy(source, target, load_sems.at[spot])
        for spot, (source, target) in enumerate(zip(sources[1:], held[1:]))
    ]
    for load in loads[:4] + cell_loads[:1] + loads[4:5] + cell_loads[1:] + loads[5:]:
        load.start()
    for load in loads[:4]:
        load.wait()

    ncat = feat_table.shape[0]
    hot = (lax.broadcasted_iota(jnp.int32, (ncat, feats), 0) == feat_ids[...]).astype(BF16)
    table = feat_table[...]
    parts = []
    for _ in range(3):
        parts.append(table.astype(BF16))
        table = table - parts[-1].astype(F32)
    femb = lax.dot_general(
        jnp.concatenate([hot] * 3, axis=0), jnp.concatenate(parts, axis=0),
        (((0,), (0,)), ((), ())), preferred_element_type=F32,
    )
    nan = nan_embed[...]
    absent = missing[...].astype(F32)

    def give(source, target, kind, row, side, peer):
        pltpu.make_async_remote_copy(
            src_ref=source.at[row, peer],
            dst_ref=target.at[row, me],
            send_sem=send_sems.at[kind, row],
            recv_sem=recv_sems.at[kind, row, side],
            device_id={"feat": peer},
            device_id_type=MESH,
        ).start()

    def spread(source, target, kind, row, spans=((1, n),)):
        def one(step, carry):
            peer = me + step
            peer = jnp.where(peer < n, peer, peer - n)
            side = jnp.where((peer >= mine) & (peer < mine + half), 0, 1)
            give(source, target, kind, row, side, peer)
            return carry

        for start, stop in spans:
            lax.fori_loop(start, stop, one, 0)

    def settle(ref, sem, row, count):
        piece = ref.at[row, pl.ds(0, count)]
        pltpu.make_async_copy(piece, piece, sem).wait()

    def arrive(ref, kind, row, side):
        settle(ref, recv_sems.at[kind, row, side], row, half - 1 + side)

    def build(row, peer):
        spot = peer * rows + row
        values = cells[peer, row].astype(F32)
        values = (values + absent[:, spot : spot + 1] * nan + femb).astype(BF16)
        tok[row, peer] = pack(values, packed)

    def tell(ahead):
        pl.semaphore_signal(
            all_sem, inc=1, device_id={"feat": me - ahead}, device_id_type=MESH
        )

    def open_outer():
        pl.semaphore_wait(barrier, n - 1)

    def tell_inner():
        tell(quarter)
        tell(half)

    def open_high():
        pl.semaphore_wait(barrier, half)

    def open_low():
        pl.semaphore_wait(barrier, quarter)
        lax.fori_loop(0, quarter, across, 0)

    def across(step, carry):
        give(tok, got, 0, 0, 1, half + lax.rem(me + step, quarter))
        return carry

    def beyond(step, carry):
        give(tok, got, 0, 0, 1, half + quarter + lax.rem(me + step, quarter))
        return carry

    def near(step, carry):
        give(tok, got, 0, 0, 0, mine + lax.rem(me - mine + step, half))
        return carry

    def wait_all():
        pl.semaphore_wait(all_sem, 1)

    def open_last():
        open_outer()
        tell_inner()

    cell_loads[0].wait()
    pl.when(part == 3)(open_last)
    pl.when(inner_high)(open_high)
    for peer in range(n):
        build(0, peer)
        if peer < half:
            pl.when(high)(lambda peer=peer: give(tok, got, 0, 0, 1, peer))
    pl.when(inner_low)(open_low)
    for row in range(1, rows):
        cell_loads[row].wait()
        for peer in range(n):
            build(row, peer)
    pl.when(part == 0)(open_outer)
    pl.when(inner_low | inner_high)(wait_all)

    lane = me - part * quarter
    far_first = (
        (1, 2 * quarter - lane),
        (3 * quarter - lane, n - lane),
        (2 * quarter - lane, 3 * quarter - lane),
        (n - lane, n),
    )

    def first_low():
        spread(tok, got, 0, 0, far_first)

    def first_rest():
        lax.fori_loop(1, half, near, 0)

    def first_beyond():
        lax.fori_loop(0, quarter, beyond, 0)

    pl.when(part == 0)(first_low)
    pl.when(part > 0)(first_rest)
    pl.when(inner_low)(first_beyond)
    for row in range(1, rows):
        pl.when(part == 0)(lambda row=row: spread(tok, got, 0, row, far_first))
        pl.when(part > 0)(lambda row=row: spread(tok, got, 0, row))
    for row in range(rows):
        got[row, pl.ds(me, 1)] = tok[row, pl.ds(me, 1)]
    for load in loads[4:]:
        load.wait()
    gain = gain_one[...]
    wqv_t[0:width] = w_qkv[:, :width].astype(F32).T.astype(BF16)
    wqv_t[width:] = w_qkv[:, 2 * width :].astype(F32).T.astype(BF16)

    head_dim = width // HEADS
    count = n * feats
    query[...] = jnp.zeros_like(query)
    value[...] = jnp.ones_like(value)

    wide = head_dim * (128 // head_dim)

    def place(row, values, column):
        values = values.reshape(n, feats, values.shape[-1]).astype(F32)
        if not packed:
            ctx[row, :, :, column : column + values.shape[-1]] = values.astype(BF16)
        elif column == 0:
            ctx[row, :, 0:feats] = values.astype(BF16)
        else:
            values = jnp.concatenate([values[:, : feats // 2], values[:, feats // 2 :]], axis=-1)
            ctx[row, :, feats : feats + feats // 2] = values.astype(BF16)

    def attention(row, carry):
        arrive(got, 0, row, 0)
        arrive(got, 0, row, 1)
        normed = cell_norm(unpack(got[row].astype(F32), feats, width, packed), gain)
        project(normed, w_qkv[:, width : 2 * width], wqv_t[...], keys, query, value, 0, count)
        scores[0][...] = score(keys, query, 0, width)
        for head in range(HEADS):
            if head + 1 < HEADS:
                scores[(head + 1) % 2][...] = score(keys, query, head + 1, width)
            turned[head * head_dim : (head + 1) * head_dim] = weigh(
                scores[head % 2][...], value, head, head_dim
            )
            if (head + 1) * head_dim == wide:
                place(row, turned[:wide].T, 0)
        place(row, turned[wide:].T, wide)
        spread(ctx, back, 1, row)
        pltpu.make_async_copy(
            ctx.at[row, me], back.at[row, me], recv_sems.at[1, row, 0]
        ).start()
        return carry

    lax.fori_loop(0, rows, attention, 0)

    before = max(rows - 1, 1)

    def finish(step, carry):
        row = jnp.where(inner_high, step // 2, step % rows)
        side = jnp.where(inner_high, step % 2, step // rows)
        row = jnp.where(part == 0, jnp.where(step < 2 * before, step % before, rows - 1), row)
        side = jnp.where(part == 0, step // before % 2, side)
        settle(back, recv_sems.at[1, row, side], row, half)
        here = pl.ds(jnp.where(side == 0, mine, other), half)
        done[row, here] = feed(
            back[row, here], tok[row, here], w_out, gain_two, w_up, w_down, feats, width, packed
        ).reshape(half, feats, width)
        return carry

    lax.fori_loop(0, 2 * rows - 1, finish, 0)
    settle(back, recv_sems.at[1, rows - 1, 1], rows - 1, half)

    for row in range(rows):
        settle(tok, send_sems.at[0, row], row, n - 1)
        settle(ctx, send_sems.at[1, row], row, n - 1)


def body(
    cells, missing, feat_ids, feat_table, nan_embed, gain_one, w_qkv, w_out, gain_two, w_up, w_down
):
    n = lax.axis_size("feat")
    all_rows, feats, width = cells.shape
    rows = all_rows // n
    packed = width == 192 and feats % 32 == 0
    piece = (feats + feats // 2, 128) if packed else (feats, width)
    buffer = pltpu.VMEM((rows, n) + piece, BF16)
    operands = (
        cells.reshape(n, rows, feats, width),
        missing.T,
        feat_ids[None],
        feat_table,
        nan_embed[None],
        gain_one[None],
        w_qkv,
        w_out,
        gain_two[None],
        w_up,
        w_down.T,
    )
    kept = pltpu.VMEM((rows, n) + piece, BF16)
    results = pl.pallas_call(
        functools.partial(kernel, n, rows, feats, width, packed),
        out_shape=[pltpu.VMEM((rows, n, feats, width), F32), kept, kept]
        + [pltpu.VMEM(x.shape, x.dtype) for x in operands[7:]],
        in_specs=[pl.BlockSpec(memory_space=pltpu.HBM)] * len(operands),
        out_specs=[pl.BlockSpec(memory_space=pltpu.VMEM)] * 7,
        scratch_shapes=[pltpu.VMEM(x.shape, x.dtype) for x in operands[:7]]
        + [
            buffer,
            buffer,
            pltpu.VMEM((2 * width, width), BF16),
            pltpu.VMEM((n * feats, width), BF16),
            pltpu.VMEM((HEADS, 128, n * feats), BF16),
            pltpu.VMEM((HEADS, width // HEADS + 16, n * feats), BF16),
            pltpu.VMEM((width, n * feats), F32),
            pltpu.VMEM((n * feats, n * feats), F32),
            pltpu.VMEM((n * feats, n * feats), F32),
            pltpu.SemaphoreType.DMA((len(operands) - 1,)),
            pltpu.SemaphoreType.DMA((rows,)),
            pltpu.SemaphoreType.DMA((2, rows)),
            pltpu.SemaphoreType.DMA((2, rows, 2)),
            pltpu.SemaphoreType.REGULAR,
        ],
        compiler_params=pltpu.CompilerParams(
            collective_id=0, has_side_effects=True, vmem_limit_bytes=LIMIT
        ),
    )(*operands)
    result = pl.pallas_call(
        functools.partial(close, n, rows, feats, width, packed),
        out_shape=jax.ShapeDtypeStruct((n, rows, feats, width), F32),
        in_specs=[pl.BlockSpec(memory_space=pltpu.VMEM)] * 7,
        out_specs=pl.BlockSpec(memory_space=pltpu.HBM),
        scratch_shapes=[
            pltpu.VMEM((n // 2, feats, width), F32),
            pltpu.SemaphoreType.DMA((rows + 1,)),
        ],
        compiler_params=pltpu.CompilerParams(vmem_limit_bytes=8 * 1024 * 1024),
    )(*results)
    return result.reshape(all_rows, feats, width)


def solution(mesh):
    in_specs = (
        P("groups", "feat", None),
        P("groups", "feat"),
        P(("groups", "feat")),
        P(),
        P(),
        P(),
        P(),
        P(),
        P(),
        P(),
        P(),
    )
    out_specs = P("groups", "feat", None)
    return jax.shard_map(body, mesh=mesh, in_specs=in_specs, out_specs=out_specs, check_vma=False)
```
